32 devices in a mesh: grp: 2 (over x), dev: 16 (over z, y, core).
Axes of the slice: x: 2, y: 2, z: 4, core: 2. Of those that a mesh axis runs over, the one named last changes fastest.
Arguments:
- line_bin: int32 [65536], P(('grp', 'dev')), may hold values from 0 to 16383, as said below
- line_slot: int32 [65536], P(('grp', 'dev')), may hold values from 0 to 31
- strength: float32 [65536], P(('grp', 'dev')), may hold values from 0.05 to 1
- line_count: int32 [32], P(('grp', 'dev')), may hold values from 1024 to 2048
- gauss_width: float32 [32], replicated, may hold values from 2 to 40
- lorentz_width: float32 [32], replicated, may hold values from 1 to 30
- mixing: float32 [32], replicated, may hold values from 0.1 to 0.9
- profile_factor: float32 [32, 257], replicated, may hold values from 0.25 to 1.75
Outputs:
- spectrum: float32 [32768], P(('grp', 'dev'))
The draws below stay inside these ranges and needn't reach their ends.
Inputs may be any that keep to these rules, and one draw needn't show every extreme that they name: `line_bin`: every line of device (g, d) (the d-th block of 2048 lines within the g-th group of 16 blocks) has a bin within (d - 2) * 1024 to (d + 3) * 1024 - 1 of its super-band.
All inputs are finite; a program needn't handle non-finite values.
Results may differ from the reference program's by a relative error of at most 0.00005.
Values sent between devices are 32-bit elements; how exact they have to be, the bound alone decides.
No kernel may reach another device: no remote copies, remote signals or barrier semaphores. Data moves between devices by JAX's collectives and lax.ppermute only.
A program may use at most 64 MiB of HBM per device.

```python
import math
import jax
import jax.numpy as jnp
from jax import lax

SLOTS = 32
WING = 128
HOP = 2
SPAN = 1024
LPD = 2048
BAND = 16384
BINS = 32768
LINES = 65536
N_GRP = 2
N_DEV = 16


def draw_line_bin(key, part):
    first, second, third = jax.random.split(jax.random.fold_in(key, 11), 3)
    devices = N_GRP * N_DEV
    owner = jnp.arange(LINES) // LPD
    member = owner % N_DEV
    centre = jax.random.randint(first, (devices,), 0, SPAN)[owner] + member * SPAN
    radius = jax.random.randint(second, (devices,), SPAN // 4, (HOP + 1) * SPAN)[owner]
    raw = jax.random.randint(third, (LINES,), 0, 2 ** 24)
    offset = raw % (2 * radius + 1) - radius
    lowest = jnp.maximum(0, (member - HOP) * SPAN)
    highest = jnp.minimum(BAND, (member + HOP + 1) * SPAN) - 1
    return jnp.clip(centre + offset, lowest, highest).astype(jnp.int32)


def place_ends(values, rng, low, high):
    extent = values.shape
    index_at = [jax.random.randint(jax.random.fold_in(rng, axis), (), 0, extent[axis]) for axis in range(len(extent))]
    values = values.at[tuple(index_at)].set(low)
    longest = extent.index(max(extent))
    index_at[longest] = (index_at[longest] + 1) % extent[longest]
    return values.at[tuple(index_at)].set(high)


def steps_of(rng, extent, shards, low, top_value):
    gain = 1.0
    for axis_at, parts in shards:
        draws = jax.random.uniform(jax.random.fold_in(jax.random.fold_in(rng, 6), axis_at), (parts,), jnp.float32, low / len(shards), top_value / len(shards))
        gain = gain * jnp.repeat(jnp.exp(draws), extent[axis_at] // parts).reshape((-1,) + (1,) * (len(extent) - 1 - axis_at))
    return gain


def setup_inputs(seed: int = 0) -> dict:
    key_list = jax.random.split(jax.random.key(seed), 9)
    return {
        "line_bin": draw_line_bin(jax.random.fold_in(key_list[8], 71), 0),
        "line_slot": place_ends(jax.random.randint(key_list[1], (LINES,), 0, SLOTS), jax.random.fold_in(key_list[1], 1), 0, SLOTS - 1).astype(jnp.int32),
        "strength": jnp.clip(jnp.exp(math.log(1.0) - 2.9957323 * jax.random.uniform(key_list[2], (LINES,), jnp.float32) ** steps_of(key_list[2], (LINES,), ((0, 32),), -0.2, 0.2)), 0.05, 1.0),
        "line_count": place_ends(jax.random.randint(key_list[3], (N_GRP * N_DEV,), LPD // 2, LPD + 1), jax.random.fold_in(key_list[3], 1), LPD // 2, LPD).astype(jnp.int32),
        "gauss_width": jnp.clip(jnp.exp(jax.random.uniform(key_list[4], (SLOTS,), jnp.float32, math.log(2.0), math.log(40.0))), 2.0, 40.0),
        "lorentz_width": jnp.clip(jnp.exp(jax.random.uniform(key_list[5], (SLOTS,), jnp.float32, math.log(1.0), math.log(30.0))), 1.0, 30.0),
        "mixing": jnp.clip(jax.random.uniform(key_list[6], (SLOTS,), jnp.float32, 0.1, 0.9), 0.1, 0.9),
        "profile_factor": jnp.clip(jax.random.uniform(key_list[7], (SLOTS, 2 * WING + 1), jnp.float32, 0.25, 1.75), 0.25, 1.75),
    }


def build_kernel(gauss_width, lorentz_width, mixing, profile_factor):
    offset = jnp.arange(-WING, WING + 1).astype(jnp.float32)
    square = offset[None, :] * offset[None, :]
    lorentz = lorentz_width[:, None] * lorentz_width[:, None] / (square + lorentz_width[:, None] * lorentz_width[:, None])
    gauss = jnp.exp(-square / (2.0 * gauss_width[:, None] * gauss_width[:, None]))
    raw = (mixing[:, None] * lorentz + (1.0 - mixing[:, None]) * gauss) * profile_factor
    return raw / jnp.sum(raw, axis=1, keepdims=True)


def reference(line_bin, line_slot, strength, line_count, gauss_width, lorentz_width, mixing, profile_factor):
    position = jnp.arange(LINES).astype(jnp.int32)
    owner = position // LPD
    group = owner // N_DEV
    live = (position % LPD) < line_count[owner]
    weight = jnp.where(live, strength, jnp.float32(0.0))
    flat = line_slot * BINS + group * BAND + line_bin
    grid = jnp.zeros((SLOTS * BINS,), jnp.float32).at[flat].add(weight).reshape(SLOTS, BINS)
    kernel = build_kernel(gauss_width, lorentz_width, mixing, profile_factor)
    spread = lax.conv_general_dilated(grid[None], kernel[:, None, :], (1,), [(WING, WING)], feature_group_count=SLOTS, precision=lax.Precision.HIGHEST)
    return jnp.sum(spread[0], axis=0)
```

```python
import jax
import jax.numpy as jnp
from jax import lax
from jax.experimental import pallas as pl
from jax.experimental.pallas import tpu as pltpu
from jax.sharding import PartitionSpec as P

HOP = 2
SPAN = 1024
LANES = 128
BLOCK = 256
AXES = ("grp", "dev")


def column(row):
    n = row.shape[1]
    here = lax.broadcasted_iota(jnp.int32, (n, n), 0)
    there = lax.broadcasted_iota(jnp.int32, (n, n), 1)
    return jnp.sum(jnp.where(here == there, row, 0.0), axis=1, keepdims=True)


def halves(value):
    high = value.astype(jnp.bfloat16)
    low = (value - high.astype(jnp.float32)).astype(jnp.bfloat16)
    return high, low


def kernel_table(gauss, lorentz, mixing, factor_ref):
    slots = gauss.shape[0]
    wing = (factor_ref.shape[1] - 1) // 2

    def profile(offset, factor):
        square = offset * offset
        width = lorentz * lorentz
        shape = mixing * (width / (square + width)) + (1.0 - mixing) * jnp.exp(
            -square / (2.0 * gauss * gauss)
        )
        return shape * factor

    lane = lax.broadcasted_iota(jnp.int32, (slots, LANES), 1)
    raw = []
    for start in range(0, 2 * wing, LANES):
        offset = (lane + (start - wing)).astype(jnp.float32)
        raw.append(profile(offset, factor_ref[:, start : start + LANES]))
    last = profile(jnp.full((slots, 1), float(wing), jnp.float32), factor_ref[:, 2 * wing :])
    total = sum(jnp.sum(part, axis=1, keepdims=True) for part in raw) + last
    raw.append(jnp.broadcast_to(last, (slots, LANES)))
    return [part / total for part in raw]


def deposit_kernel(
    count_ref, bin_ref, slot_ref, strength_ref, gauss_ref, lorentz_ref, mixing_ref, factor_ref, out_ref
):
    slots = gauss_ref.shape[1]
    pieces = (factor_ref.shape[1] - 1) // LANES
    lines = bin_ref.shape[1]
    reach_rows = (2 * HOP + 1) * SPAN // LANES
    rows = -(-(reach_rows + pieces) // 16) * 16
    bf16 = jnp.bfloat16

    table = kernel_table(
        column(gauss_ref[...]), column(lorentz_ref[...]), column(mixing_ref[...]), factor_ref
    )
    table = jnp.concatenate(table, axis=1)
    high, low = halves(table)
    weights = jnp.concatenate([high, low, high, low], axis=0)
    ones = (lax.broadcasted_iota(jnp.int32, (16, LANES), 0) == 0).astype(jnp.float32).astype(bf16)
    weights = jnp.concatenate(
        [
            jnp.concatenate([weights, jnp.zeros((4 * slots, LANES), bf16)], axis=1),
            jnp.concatenate([jnp.zeros((16, table.shape[1]), bf16), ones], axis=1),
        ],
        axis=0,
    )

    anchor = (lax.axis_index("dev") - HOP) * SPAN
    count = count_ref[0]
    slot_ids = lax.broadcasted_iota(jnp.int32, (slots, BLOCK), 0)
    row_ids = lax.broadcasted_iota(jnp.int32, (rows, BLOCK), 0)
    lane = lax.broadcasted_iota(jnp.int32, (BLOCK, LANES), 1)
    acc = jnp.zeros((rows, 2 * LANES), jnp.float32)
    for start in range(0, lines, BLOCK):
        at = slice(start, start + BLOCK)
        where = bin_ref[:, at] - anchor
        row, col = where >> 7, where & (LANES - 1)
        live = lax.broadcasted_iota(jnp.int32, (1, BLOCK), 1) + start < count
        weight = jnp.where(live, strength_ref[:, at], 0.0)
        chosen = jnp.where(slot_ids == slot_ref[:, at], weight, 0.0)
        chosen_high, chosen_low = halves(chosen)
        cols = jnp.broadcast_to(col.astype(jnp.float32), (16, BLOCK)).astype(bf16)
        picks = jnp.concatenate([chosen_high, chosen_high, chosen_low, chosen_low, cols], axis=0)
        spread = lax.dot_general(
            picks, weights, (((0,), (0,)), ((), ())), preferred_element_type=jnp.float32
        )
        col = spread[:, (pieces + 1) * LANES :].astype(jnp.int32)
        index = (col - lane) & (LANES - 1)
        turned = [
            jnp.take_along_axis(
                spread[:, k * LANES : (k + 1) * LANES], index, axis=1, mode="promise_in_bounds"
            )
            for k in range(pieces)
        ]
        last = spread[:, pieces * LANES : (pieces + 1) * LANES]
        after, here = lane > col, lane == col
        for k in range(pieces + 1):
            if k == 0:
                value = jnp.where(after, turned[pieces - 1], jnp.where(here, last, 0.0))
            elif k == pieces:
                value = jnp.where(after, 0.0, turned[0])
            else:
                value = jnp.where(after, turned[pieces - 1 - k], turned[pieces - k])
            onto = (row_ids == row + k).astype(jnp.float32).astype(bf16)
            acc += jnp.dot(
                onto, jnp.concatenate(halves(value), axis=1), preferred_element_type=jnp.float32
            )
    out_ref[...] = acc[:, :LANES] + acc[:, LANES:]


def local_spectrum(line_bin, line_slot, strength, line_count, gauss, lorentz, mixing, factor):
    lines, slots = line_bin.shape[0], gauss.shape[0]
    pieces = (factor.shape[1] - 1) // LANES
    reach_rows = (2 * HOP + 1) * SPAN // LANES
    rows = -(-(reach_rows + pieces) // 16) * 16
    vmem = pl.BlockSpec(memory_space=pltpu.VMEM)
    return pl.pallas_call(
        deposit_kernel,
        out_shape=jax.ShapeDtypeStruct((rows, LANES), jnp.float32),
        in_specs=[pl.BlockSpec(memory_space=pltpu.SMEM)] + [vmem] * 7,
        out_specs=vmem,
    )(
        line_count,
        line_bin.reshape(1, lines),
        line_slot.reshape(1, lines),
        strength.reshape(1, lines),
        gauss.reshape(1, slots),
        lorentz.reshape(1, slots),
        mixing.reshape(1, slots),
        factor,
    )


def body(line_bin, line_slot, strength, line_count, gauss, lorentz, mixing, factor):
    spectrum = local_spectrum(line_bin, line_slot, strength, line_count, gauss, lorentz, mixing, factor)
    devices = lax.axis_size(AXES)
    me = lax.axis_index(AXES)
    wing_rows = (factor.shape[1] - 1) // 2 // LANES
    span_rows = SPAN // LANES
    far = HOP + 1
    whole = jnp.zeros(((devices + 2 * far) * span_rows, LANES), jnp.float32)
    used = (2 * HOP + 1) * span_rows + 2 * wing_rows
    whole = lax.dynamic_update_slice(
        whole, spectrum[:used], ((me + far - HOP) * span_rows - wing_rows, 0)
    )
    parts = whole[far * span_rows : (far + devices) * span_rows].reshape(devices, span_rows, LANES)
    parts = lax.all_to_all(parts, AXES, 0, 0, tiled=True)
    return jnp.sum(parts, axis=0).reshape(SPAN)


def solution(mesh):
    in_specs = (P(AXES),) * 4 + (P(),) * 4
    return jax.shard_map(body, mesh=mesh, in_specs=in_specs, out_specs=P(AXES), check_vma=False)
```

```python
import jax
import jax.numpy as jnp
from jax import lax
from jax.experimental import pallas as pl
from jax.experimental.pallas import tpu as pltpu
from jax.sharding import PartitionSpec as P

HOP = 2
SPAN = 1024
LANES = 128
BLOCK = 256
AXES = ("grp", "dev")


def column(row):
    n = row.shape[1]
    here = lax.broadcasted_iota(jnp.int32, (n, n), 0)
    there = lax.broadcasted_iota(jnp.int32, (n, n), 1)
    return jnp.sum(jnp.where(here == there, row, 0.0), axis=1, keepdims=True)


def halves(value):
    high = value.astype(jnp.bfloat16)
    low = (value - high.astype(jnp.float32)).astype(jnp.bfloat16)
    return high, low


def kernel_table(gauss, lorentz, mixing, factor_ref):
    slots = gauss.shape[0]
    wing = (factor_ref.shape[1] - 1) // 2

    def profile(offset, factor):
        square = offset * offset
        width = lorentz * lorentz
        shape = mixing * (width / (square + width)) + (1.0 - mixing) * jnp.exp(
            -square / (2.0 * gauss * gauss)
        )
        return shape * factor

    lane = lax.broadcasted_iota(jnp.int32, (slots, LANES), 1)
    raw = []
    for start in range(0, 2 * wing, LANES):
        offset = (lane + (start - wing)).astype(jnp.float32)
        raw.append(profile(offset, factor_ref[:, start : start + LANES]))
    last = profile(jnp.full((slots, 1), float(wing), jnp.float32), factor_ref[:, 2 * wing :])
    total = sum(jnp.sum(part, axis=1, keepdims=True) for part in raw) + last
    raw.append(jnp.broadcast_to(last, (slots, LANES)))
    return [part / total for part in raw]


def deposit_kernel(
    count_ref, bin_ref, slot_ref, strength_ref, gauss_ref, lorentz_ref, mixing_ref, factor_ref, out_ref, acc_ref
):
    slots = gauss_ref.shape[1]
    pieces = (factor_ref.shape[1] - 1) // LANES
    lines = bin_ref.shape[1]
    reach_rows = (2 * HOP + 1) * SPAN // LANES
    rows = -(-(reach_rows + pieces) // 16) * 16
    bf16 = jnp.bfloat16

    table = kernel_table(
        column(gauss_ref[...]), column(lorentz_ref[...]), column(mixing_ref[...]), factor_ref
    )
    table = jnp.concatenate(table, axis=1)
    high, low = halves(table)
    weights = jnp.concatenate([high, low, high, low], axis=0)
    ones = (lax.broadcasted_iota(jnp.int32, (16, LANES), 0) == 0).astype(jnp.float32).astype(bf16)
    weights = jnp.concatenate(
        [
            jnp.concatenate([weights, jnp.zeros((4 * slots, LANES), bf16)], axis=1),
            jnp.concatenate([jnp.zeros((16, table.shape[1]), bf16), ones], axis=1),
        ],
        axis=0,
    )

    anchor = (lax.axis_index("dev") - HOP) * SPAN
    count = count_ref[0]
    slot_ids = lax.broadcasted_iota(jnp.int32, (slots, BLOCK), 0)
    row_ids = lax.broadcasted_iota(jnp.int32, (rows, BLOCK), 0)
    lane = lax.broadcasted_iota(jnp.int32, (BLOCK, LANES), 1)
    acc = jnp.zeros((rows, 2 * LANES), jnp.float32)
    for start in range(0, lines, BLOCK):
        at = slice(start, start + BLOCK)
        where = bin_ref[:, at] - anchor
        row, col = where >> 7, where & (LANES - 1)
        live = lax.broadcasted_iota(jnp.int32, (1, BLOCK), 1) + start < count
        weight = jnp.where(live, strength_ref[:, at], 0.0)
        chosen = jnp.where(slot_ids == slot_ref[:, at], weight, 0.0)
        chosen_high, chosen_low = halves(chosen)
        cols = jnp.broadcast_to(col.astype(jnp.float32), (16, BLOCK)).astype(bf16)
        picks = jnp.concatenate([chosen_high, chosen_high, chosen_low, chosen_low, cols], axis=0)
        spread = lax.dot_general(
            picks, weights, (((0,), (0,)), ((), ())), preferred_element_type=jnp.float32
        )
        col = spread[:, (pieces + 1) * LANES :].astype(jnp.int32)
        index = (col - lane) & (LANES - 1)
        turned = [
            jnp.take_along_axis(
                spread[:, k * LANES : (k + 1) * LANES], index, axis=1, mode="promise_in_bounds"
            )
            for k in range(pieces)
        ]
        last = spread[:, pieces * LANES : (pieces + 1) * LANES]
        after, here = lane > col, lane == col
        for k in range(pieces + 1):
            if k == 0:
                value = jnp.where(after, turned[pieces - 1], jnp.where(here, last, 0.0))
            elif k == pieces:
                value = jnp.where(after, 0.0, turned[0])
            else:
                value = jnp.where(after, turned[pieces - 1 - k], turned[pieces - k])
            onto = (row_ids == row + k).astype(jnp.float32).astype(bf16)
            acc += jnp.dot(
                onto, jnp.concatenate(halves(value), axis=1), preferred_element_type=jnp.float32
            )
    span_rows, wing_rows = SPAN // LANES, pieces // 2
    shift = (HOP + 1) * span_rows - HOP * span_rows - wing_rows
    acc_ref[:shift] = jnp.zeros((shift, LANES), jnp.float32)
    acc_ref[shift : shift + rows] = acc[:, :LANES] + acc[:, LANES:]
    end = shift + reach_rows + 2 * wing_rows
    acc_ref[end:] = jnp.zeros((acc_ref.shape[0] - end, LANES), jnp.float32)
    out_ref[...] = jnp.zeros_like(out_ref)
    me = lax.axis_index(AXES)
    for step in range(-HOP - 1, HOP + 2):
        at = me + step

        @pl.when((at >= 0) & (at < out_ref.shape[0]))
        def _():
            first = (step + HOP + 1) * span_rows
            out_ref[at] = acc_ref[first : first + span_rows]


def span_blocks(line_bin, line_slot, strength, line_count, gauss, lorentz, mixing, factor):
    lines, slots = line_bin.shape[0], gauss.shape[0]
    span_rows = SPAN // LANES
    rows = -(-((2 * HOP + 3) * span_rows + LANES) // 16) * 16
    vmem = pl.BlockSpec(memory_space=pltpu.VMEM)
    return pl.pallas_call(
        deposit_kernel,
        out_shape=pltpu.VMEM((lax.axis_size(AXES), span_rows, LANES), jnp.float32),
        in_specs=[pl.BlockSpec(memory_space=pltpu.SMEM)] + [vmem] * 7,
        out_specs=vmem,
        scratch_shapes=[pltpu.VMEM((rows, LANES), jnp.float32)],
    )(
        line_count,
        line_bin.reshape(1, lines),
        line_slot.reshape(1, lines),
        strength.reshape(1, lines),
        gauss.reshape(1, slots),
        lorentz.reshape(1, slots),
        mixing.reshape(1, slots),
        factor,
    )


def body(line_bin, line_slot, strength, line_count, gauss, lorentz, mixing, factor):
    parts = span_blocks(line_bin, line_slot, strength, line_count, gauss, lorentz, mixing, factor)
    parts = lax.all_to_all(parts, AXES, 0, 0, tiled=True)
    return jnp.sum(parts, axis=0).reshape(SPAN)


def solution(mesh):
    in_specs = (P(AXES),) * 4 + (P(),) * 4
    return jax.shard_map(body, mesh=mesh, in_specs=in_specs, out_specs=P(AXES), check_vma=False)
```

```python
import jax
import jax.numpy as jnp
from jax import lax
from jax.experimental import pallas as pl
from jax.experimental.pallas import tpu as pltpu
from jax.sharding import PartitionSpec as P

HOP = 2
SPAN = 1024
LANES = 128
BLOCK = 256
STAGE = 256
AXES = ("grp", "dev")


def column(row):
    n = row.shape[1]
    here = lax.broadcasted_iota(jnp.int32, (n, n), 0)
    there = lax.broadcasted_iota(jnp.int32, (n, n), 1)
    return jnp.sum(jnp.where(here == there, row, 0.0), axis=1, keepdims=True)


def halves(value):
    high = value.astype(jnp.bfloat16)
    low = (value - high.astype(jnp.float32)).astype(jnp.bfloat16)
    return high, low


def pick_lanes(value, index):
    numbers = lax.GatherDimensionNumbers(
        offset_dims=(),
        collapsed_slice_dims=(1,),
        start_index_map=(1,),
        operand_batching_dims=(0,),
        start_indices_batching_dims=(0,),
    )
    return lax.gather(
        value, index[..., None], numbers, (1, 1), mode=lax.GatherScatterMode.PROMISE_IN_BOUNDS
    )


def kernel_table(gauss, lorentz, mixing, factor_ref):
    slots = gauss.shape[0]
    wing = (factor_ref.shape[1] - 1) // 2

    def profile(offset, factor):
        square = offset * offset
        width = lorentz * lorentz
        shape = mixing * (width / (square + width)) + (1.0 - mixing) * jnp.exp(
            -square / (2.0 * gauss * gauss)
        )
        return shape * factor

    lane = lax.broadcasted_iota(jnp.int32, (slots, LANES), 1)
    raw = []
    for start in range(0, 2 * wing, LANES):
        offset = (lane + (start - wing)).astype(jnp.float32)
        raw.append(profile(offset, factor_ref[:, start : start + LANES]))
    last = profile(jnp.full((slots, 1), float(wing), jnp.float32), factor_ref[:, 2 * wing :])
    total = sum(jnp.sum(part, axis=1, keepdims=True) for part in raw) + last
    return jnp.concatenate(raw, axis=1) / total, last / total


def deposit_kernel(
    count_ref, bin_ref, slot_ref, strength_ref, gauss_ref, lorentz_ref, mixing_ref, factor_ref, give_ref, half_ref, acc_ref, spread_ref
):
    slots = gauss_ref.shape[1]
    pieces = (factor_ref.shape[1] - 1) // LANES
    lines = bin_ref.shape[1]
    reach_rows = (2 * HOP + 1) * SPAN // LANES
    rows = -(-(reach_rows + pieces) // 16) * 16
    bf16 = jnp.bfloat16

    table, last = kernel_table(
        column(gauss_ref[...]), column(lorentz_ref[...]), column(mixing_ref[...]), factor_ref
    )
    high, low = halves(table)
    weights = jnp.concatenate([high, low, high, low], axis=0)
    aux = lax.broadcasted_iota(jnp.int32, (16, LANES), 0)
    aux_lane = lax.broadcasted_iota(jnp.int32, (16, LANES), 1)
    steps = jnp.where(aux == 0, 1, jnp.where(aux == 1, LANES - aux_lane, 0))
    steps = steps.astype(jnp.float32).astype(bf16)
    weights = jnp.concatenate(
        [
            jnp.concatenate([weights, jnp.zeros((4 * slots, LANES), bf16)], axis=1),
            jnp.concatenate([jnp.zeros((16, table.shape[1]), bf16), steps], axis=1),
        ],
        axis=0,
    )

    anchor = (lax.axis_index("dev") - HOP) * SPAN
    count = count_ref[0]
    slot_ids = lax.broadcasted_iota(jnp.int32, (slots, STAGE), 0)
    row_ids = lax.broadcasted_iota(jnp.int32, (rows, BLOCK), 0)
    aux_ids = lax.broadcasted_iota(jnp.int32, (16, STAGE), 0)
    zero, one = jnp.zeros((BLOCK, LANES), bf16), jnp.ones((BLOCK, LANES), bf16)
    ends_at = []
    for start in range(0, lines, STAGE):
        at = slice(start, start + STAGE)
        col = (bin_ref[:, at] - anchor) & (LANES - 1)
        live = lax.broadcasted_iota(jnp.int32, (1, STAGE), 1) + start < count
        weight = jnp.where(live, strength_ref[:, at], 0.0)
        chosen = jnp.where(slot_ids == slot_ref[:, at], weight, 0.0)
        ends_at.append(jnp.sum(chosen * last, axis=0, keepdims=True))
        chosen_high, chosen_low = halves(chosen)
        aux = jnp.where(aux_ids == 0, col, jnp.where(aux_ids == 1, 1, 0))
        aux = aux.astype(jnp.float32).astype(bf16)
        picks = jnp.concatenate([chosen_high, chosen_high, chosen_low, chosen_low, aux], axis=0)
        spread_ref[at, :] = lax.dot_general(
            picks, weights, (((0,), (0,)), ((), ())), preferred_element_type=jnp.float32
        )
    ends_at = jnp.concatenate(ends_at, axis=1)
    acc = jnp.zeros((rows, 2 * LANES), jnp.float32)
    ends = jnp.zeros((2 * rows, LANES), jnp.float32)
    for start in range(0, lines, BLOCK):
        at = slice(start, start + BLOCK)
        row = (bin_ref[:, at] - anchor) >> 7
        step = spread_ref[at, pieces * LANES :]
        index = step.astype(jnp.int32) & (LANES - 1)
        turned = [
            halves(pick_lanes(spread_ref[at, k * LANES : (k + 1) * LANES], index))
            for k in range(pieces)
        ]
        step = step.astype(bf16)
        after, here = step < LANES, step == LANES
        for k in range(pieces + 1):
            past = turned[pieces - 1 - k] if k < pieces else (zero, zero)
            upto = turned[pieces - k] if k > 0 else (zero, zero)
            value = [jnp.where(after, a, b) for a, b in zip(past, upto)]
            onto = (row_ids == row + k).astype(jnp.float32).astype(bf16)
            acc += jnp.dot(
                onto, jnp.concatenate(value, axis=1), preferred_element_type=jnp.float32
            )
        onto = jnp.concatenate(halves(jnp.where(row_ids == row, ends_at[:, at], 0.0)), axis=0)
        ends += jnp.dot(onto, jnp.where(here, one, zero), preferred_element_type=jnp.float32)
    acc = acc[:, :LANES] + acc[:, LANES:] + ends[:rows] + ends[rows:]

    span_rows, wing_rows = SPAN // LANES, pieces // 2
    shift = (HOP + 1) * span_rows - HOP * span_rows - wing_rows
    acc_ref[:shift] = jnp.zeros((shift, LANES), jnp.float32)
    acc_ref[shift : shift + rows] = acc
    end = shift + reach_rows + 2 * wing_rows
    acc_ref[end:] = jnp.zeros((acc_ref.shape[0] - end, LANES), jnp.float32)
    odd = lax.rem(lax.axis_index(AXES), 2)
    far = HOP + 1
    give = pl.multiple_of((1 - odd) * (far + 1) * span_rows, span_rows)
    keep = pl.multiple_of(odd * far * span_rows, span_rows)
    give_ref[...] = acc_ref[pl.ds(give, far * span_rows)]
    half_ref[...] = acc_ref[pl.ds(keep, (far + 1) * span_rows)]


def span_sums(line_bin, line_slot, strength, line_count, gauss, lorentz, mixing, factor):
    lines, slots = line_bin.shape[0], gauss.shape[0]
    span_rows = SPAN // LANES
    rows = -(-((2 * HOP + 3) * span_rows + LANES) // 16) * 16
    vmem = pl.BlockSpec(memory_space=pltpu.VMEM)
    return pl.pallas_call(
        deposit_kernel,
        out_shape=[
            pltpu.VMEM(((HOP + 1) * span_rows, LANES), jnp.float32),
            pltpu.VMEM(((HOP + 2) * span_rows, LANES), jnp.float32),
        ],
        in_specs=[pl.BlockSpec(memory_space=pltpu.SMEM)] + [vmem] * 7,
        out_specs=[vmem] * 2,
        scratch_shapes=[
            pltpu.VMEM((rows, LANES), jnp.float32),
            pltpu.VMEM((lines, factor.shape[1] - 1 + LANES), jnp.float32),
        ],
    )(
        line_count,
        line_bin.reshape(1, lines),
        line_slot.reshape(1, lines),
        strength.reshape(1, lines),
        gauss.reshape(1, slots),
        lorentz.reshape(1, slots),
        mixing.reshape(1, slots),
        factor,
    )


def exchanges(groups, members):
    count = groups * members
    pair = {i: i ^ 1 for i in range(count)}
    near = {i: i + 1 if i % 2 else i - 1 for i in range(count)}
    far = {i: i + 3 if i % 2 else i - 3 for i in range(count)}
    for moves in (near, far):
        for i, j in moves.items():
            if not 0 <= j < count:
                moves[i] = i
    for b in range(members, count, members):
        near.update({b - 3: b, b - 1: b + 1, b: b - 2, b + 2: b - 1})
        far.update({b - 5: b - 1, b - 3: b - 2, b - 1: b - 3, b: b + 2, b + 2: b + 1, b + 4: b})
    for moves in (pair, near, far):
        assert sorted(moves.values()) == list(range(count))
    return [sorted(moves.items()) for moves in (pair, near, far)]


def body(line_bin, line_slot, strength, line_count, gauss, lorentz, mixing, factor):
    groups, members = lax.axis_size("grp"), lax.axis_size("dev")
    pair, near, far = exchanges(groups, members)
    rows = SPAN // LANES
    me, last = lax.axis_index(AXES), groups * members - 1
    group, place = lax.axis_index("grp"), lax.axis_index("dev")
    odd = me % 2 == 1
    even = ~odd

    def before(k):
        return (place == members - k) & (group < groups - 1)

    def behind(k):
        return (place == k) & (group > 0)

    def part(value, first):
        return value[first * rows : (first + 1) * rows]

    give, half = span_sums(line_bin, line_slot, strength, line_count, gauss, lorentz, mixing, factor)
    got = lax.ppermute(give, AXES, pair)
    zero = jnp.zeros((rows, LANES), jnp.float32)
    half = half + jnp.where(
        even, jnp.concatenate([zero, got], axis=0), jnp.concatenate([got, zero], axis=0)
    )
    padded = jnp.concatenate([half, zero], axis=0)
    first = jnp.where(before(3), 3, jnp.where(behind(0), 2, jnp.where(behind(2), 0, 1)))
    to_near = lax.dynamic_slice(padded, (first * rows, 0), (2 * rows, LANES))
    first = jnp.where(before(3) | behind(2), 1, jnp.where(odd, 3, 0))
    to_far = lax.dynamic_slice(padded, (first * rows, 0), (2 * rows, LANES))
    near = lax.ppermute(to_near, AXES, near)
    far = lax.ppermute(to_far, AXES, far)

    inner_even = even & (me > 0) & ~before(2)
    inner_odd = odd & (me < last) & ~before(1)
    outer = before(1) | before(3) | behind(0) | behind(1) | behind(2)
    reached = jnp.where(even, me > 2, me < last - 2) & ~outer
    own = (
        jnp.where(even, part(half, 3), part(half, 0))
        + jnp.where(inner_even | before(1), part(near, 0), 0.0)
        + jnp.where(inner_odd & ~behind(1), part(near, 1), 0.0)
        + jnp.where(reached, part(far, 0), 0.0)
        + jnp.where(behind(1), part(far, 1), 0.0)
    )
    other = (
        jnp.where(inner_odd | before(2), part(near, 0), 0.0)
        + jnp.where(inner_even & ~behind(0), part(near, 1), 0.0)
        + jnp.where(before(1) | behind(0) | behind(1), part(far, 0), 0.0)
        + jnp.where(before(2), part(far, 1), 0.0)
    )
    got = lax.ppermute(other, AXES, pair)
    return (own + got).reshape(SPAN)


def solution(mesh):
    in_specs = (P(AXES),) * 4 + (P(),) * 4
    return jax.shard_map(body, mesh=mesh, in_specs=in_specs, out_specs=P(AXES), check_vma=False)
```

```python
import jax
import jax.numpy as jnp
from jax import lax
from jax.experimental import pallas as pl
from jax.experimental.pallas import tpu as pltpu
from jax.sharding import PartitionSpec as P

HOP = 2
SPAN = 1024
LANES = 128
BLOCK = 256
STAGE = 256
AXES = ("grp", "dev")


def column(row):
    n = row.shape[1]
    here = lax.broadcasted_iota(jnp.int32, (n, n), 0)
    there = lax.broadcasted_iota(jnp.int32, (n, n), 1)
    return jnp.sum(jnp.where(here == there, row, 0.0), axis=1, keepdims=True)


def halves(value):
    high = value.astype(jnp.bfloat16)
    low = (value - high.astype(jnp.float32)).astype(jnp.bfloat16)
    return high, low


def pick_lanes(value, index):
    numbers = lax.GatherDimensionNumbers(
        offset_dims=(),
        collapsed_slice_dims=(1,),
        start_index_map=(1,),
        operand_batching_dims=(0,),
        start_indices_batching_dims=(0,),
    )
    return lax.gather(
        value, index[..., None], numbers, (1, 1), mode=lax.GatherScatterMode.PROMISE_IN_BOUNDS
    )


def kernel_table(gauss, lorentz, mixing, factor_ref):
    slots = gauss.shape[0]
    wing = (factor_ref.shape[1] - 1) // 2

    def profile(offset, factor):
        square = offset * offset
        width = lorentz * lorentz
        shape = mixing * (width / (square + width)) + (1.0 - mixing) * jnp.exp(
            -square / (2.0 * gauss * gauss)
        )
        return shape * factor

    lane = lax.broadcasted_iota(jnp.int32, (slots, LANES), 1)
    raw = []
    for start in range(0, 2 * wing, LANES):
        offset = (lane + (start - wing)).astype(jnp.float32)
        raw.append(profile(offset, factor_ref[:, start : start + LANES]))
    last = profile(jnp.full((slots, 1), float(wing), jnp.float32), factor_ref[:, 2 * wing :])
    total = sum(jnp.sum(part, axis=1, keepdims=True) for part in raw) + last
    return jnp.concatenate(raw, axis=1) / total, last / total


def deposit_kernel(
    count_ref, bin_ref, slot_ref, strength_ref, gauss_ref, lorentz_ref, mixing_ref, factor_ref, give_ref, half_ref, acc_ref, spread_ref
):
    slots = gauss_ref.shape[1]
    pieces = (factor_ref.shape[1] - 1) // LANES
    lines = bin_ref.shape[1]
    reach_rows = (2 * HOP + 1) * SPAN // LANES
    rows = -(-(reach_rows + pieces) // 16) * 16
    bf16 = jnp.bfloat16

    table, last = kernel_table(
        column(gauss_ref[...]), column(lorentz_ref[...]), column(mixing_ref[...]), factor_ref
    )
    high, low = halves(table)
    weights = jnp.concatenate([high, low, high, low], axis=0)
    aux = lax.broadcasted_iota(jnp.int32, (16, LANES), 0)
    aux_lane = lax.broadcasted_iota(jnp.int32, (16, LANES), 1)
    steps = jnp.where(aux == 0, 1, jnp.where(aux == 1, LANES - aux_lane, 0))
    steps = steps.astype(jnp.float32).astype(bf16)
    weights = jnp.concatenate(
        [
            jnp.concatenate([weights, jnp.zeros((4 * slots, LANES), bf16)], axis=1),
            jnp.concatenate([jnp.zeros((16, table.shape[1]), bf16), steps], axis=1),
        ],
        axis=0,
    )

    anchor = (lax.axis_index("dev") - HOP) * SPAN
    count = count_ref[0]
    slot_ids = lax.broadcasted_iota(jnp.int32, (slots, STAGE), 0)
    row_ids = lax.broadcasted_iota(jnp.int32, (rows, BLOCK), 0)
    aux_ids = lax.broadcasted_iota(jnp.int32, (16, STAGE), 0)
    zero, one = jnp.zeros((BLOCK, LANES), bf16), jnp.ones((BLOCK, LANES), bf16)
    ends_at = []
    for start in range(0, lines, STAGE):
        at = slice(start, start + STAGE)
        col = (bin_ref[:, at] - anchor) & (LANES - 1)
        live = lax.broadcasted_iota(jnp.int32, (1, STAGE), 1) + start < count
        weight = jnp.where(live, strength_ref[:, at], 0.0)
        chosen = jnp.where(slot_ids == slot_ref[:, at], weight, 0.0)
        ends_at.append(jnp.sum(chosen * last, axis=0, keepdims=True))
        chosen_high, chosen_low = halves(chosen)
        aux = jnp.where(aux_ids == 0, col, jnp.where(aux_ids == 1, 1, 0))
        aux = aux.astype(jnp.float32).astype(bf16)
        picks = jnp.concatenate([chosen_high, chosen_high, chosen_low, chosen_low, aux], axis=0)
        spread_ref[at, :] = lax.dot_general(
            picks, weights, (((0,), (0,)), ((), ())), preferred_element_type=jnp.float32
        )
    ends_at = jnp.concatenate(ends_at, axis=1)
    acc = jnp.zeros((rows, 2 * LANES), jnp.float32)
    ends = jnp.zeros((2 * rows, LANES), jnp.float32)
    for start in range(0, lines, BLOCK):
        at = slice(start, start + BLOCK)
        row = (bin_ref[:, at] - anchor) >> 7
        step = spread_ref[at, pieces * LANES :]
        index = step.astype(jnp.int32) & (LANES - 1)
        turned = [
            halves(pick_lanes(spread_ref[at, k * LANES : (k + 1) * LANES], index))
            for k in range(pieces)
        ]
        step = step.astype(bf16)
        after, here = step < LANES, step == LANES
        for k in range(pieces + 1):
            past = turned[pieces - 1 - k] if k < pieces else (zero, zero)
            upto = turned[pieces - k] if k > 0 else (zero, zero)
            value = [jnp.where(after, a, b) for a, b in zip(past, upto)]
            onto = (row_ids == row + k).astype(jnp.float32).astype(bf16)
            acc += jnp.dot(
                onto, jnp.concatenate(value, axis=1), preferred_element_type=jnp.float32
            )
        onto = jnp.concatenate(halves(jnp.where(row_ids == row, ends_at[:, at], 0.0)), axis=0)
        ends += jnp.dot(onto, jnp.where(here, one, zero), preferred_element_type=jnp.float32)
    acc = acc[:, :LANES] + acc[:, LANES:] + ends[:rows] + ends[rows:]

    span_rows, wing_rows = SPAN // LANES, pieces // 2
    shift = (HOP + 1) * span_rows - HOP * span_rows - wing_rows
    acc_ref[:shift] = jnp.zeros((shift, LANES), jnp.float32)
    acc_ref[shift : shift + rows] = acc
    end = shift + reach_rows + 2 * wing_rows
    acc_ref[end:] = jnp.zeros((acc_ref.shape[0] - end, LANES), jnp.float32)
    odd = lax.rem(lax.axis_index(AXES), 2)
    far = HOP + 1
    give = pl.multiple_of((1 - odd) * (far + 1) * span_rows, span_rows)
    keep = pl.multiple_of(odd * far * span_rows, span_rows)
    give_ref[...] = acc_ref[pl.ds(give, far * span_rows)]
    half_ref[...] = acc_ref[pl.ds(keep, (far + 1) * span_rows)]


def span_sums(line_bin, line_slot, strength, line_count, gauss, lorentz, mixing, factor):
    lines, slots = line_bin.shape[0], gauss.shape[0]
    span_rows = SPAN // LANES
    rows = -(-((2 * HOP + 3) * span_rows + LANES) // 16) * 16
    vmem = pl.BlockSpec(memory_space=pltpu.VMEM)
    return pl.pallas_call(
        deposit_kernel,
        out_shape=[
            pltpu.VMEM(((HOP + 1) * span_rows, LANES), jnp.float32),
            pltpu.VMEM(((HOP + 2) * span_rows, LANES), jnp.float32),
        ],
        in_specs=[pl.BlockSpec(memory_space=pltpu.SMEM)] + [vmem] * 7,
        out_specs=[vmem] * 2,
        scratch_shapes=[
            pltpu.VMEM((rows, LANES), jnp.float32),
            pltpu.VMEM((lines, factor.shape[1] - 1 + LANES), jnp.float32),
        ],
    )(
        line_count,
        line_bin.reshape(1, lines),
        line_slot.reshape(1, lines),
        strength.reshape(1, lines),
        gauss.reshape(1, slots),
        lorentz.reshape(1, slots),
        mixing.reshape(1, slots),
        factor,
    )


def exchanges(groups, members):
    count = groups * members
    pair = [(i, i ^ 1) for i in range(count)]
    near = [(i, i + (1 if i % 2 else -1)) for i in range(count)]
    far = [(i, i + (3 if i % 2 else -3)) for i in range(count)]
    near, far = (
        [(i, j) for i, j in moves if 0 <= j < count and i // members == j // members]
        for moves in (near, far)
    )
    cross = []
    for b in range(members, count, members):
        cross += [(b - 1, b), (b - 3, b + 1), (b, b - 1), (b + 2, b - 2)]
    return pair, near, far, cross


def body(line_bin, line_slot, strength, line_count, gauss, lorentz, mixing, factor):
    groups, members = lax.axis_size("grp"), lax.axis_size("dev")
    pair, near, far, cross = exchanges(groups, members)
    rows = SPAN // LANES
    group, place = lax.axis_index("grp"), lax.axis_index("dev")
    odd = place % 2 == 1
    even = ~odd

    def before(k):
        return (place == members - k) & (group < groups - 1)

    def behind(k):
        return (place == k) & (group > 0)

    def part(value, first):
        return value[first * rows : (first + 1) * rows]

    give, half = span_sums(line_bin, line_slot, strength, line_count, gauss, lorentz, mixing, factor)
    got = lax.ppermute(give, AXES, pair)
    zero = jnp.zeros((rows, LANES), jnp.float32)
    half = half + jnp.where(
        even, jnp.concatenate([zero, got], axis=0), jnp.concatenate([got, zero], axis=0)
    )
    to_cross = jnp.where(
        before(3),
        part(half, 3),
        jnp.where(before(1), part(half, 1), jnp.where(behind(0), part(half, 2), part(half, 0))),
    )
    cross = lax.ppermute(to_cross, AXES, cross)
    near = lax.ppermute(half[rows : 3 * rows], AXES, near)
    far = lax.ppermute(jnp.where(even, part(half, 0), part(half, 3)), AXES, far)
    edge = before(1) | behind(0)
    own = jnp.where(even, part(half, 3) + part(near, 0), part(half, 0) + part(near, 1))
    own = own + far + jnp.where(edge, cross, 0.0)
    other = jnp.where(even, part(near, 1), part(near, 0)) + jnp.where(edge, 0.0, cross)
    got = lax.ppermute(other, AXES, pair)
    return (own + got).reshape(SPAN)


def solution(mesh):
    in_specs = (P(AXES),) * 4 + (P(),) * 4
    return jax.shard_map(body, mesh=mesh, in_specs=in_specs, out_specs=P(AXES), check_vma=False)
```

```python
import jax
import jax.numpy as jnp
from jax import lax
from jax.experimental import pallas as pl
from jax.experimental.pallas import tpu as pltpu
from jax.sharding import PartitionSpec as P

HOP = 2
SPAN = 1024
LANES = 128
BLOCK = 128
STAGE = 512
AXES = ("grp", "dev")


def column(row):
    n = row.shape[1]
    here = lax.broadcasted_iota(jnp.int32, (n, n), 0)
    there = lax.broadcasted_iota(jnp.int32, (n, n), 1)
    return jnp.sum(jnp.where(here == there, row, 0.0), axis=1, keepdims=True)


def halves(value):
    high = value.astype(jnp.bfloat16)
    low = (value - high.astype(jnp.float32)).astype(jnp.bfloat16)
    return high, low


def pick_lanes(value, index):
    numbers = lax.GatherDimensionNumbers(
        offset_dims=(),
        collapsed_slice_dims=(1,),
        start_index_map=(1,),
        operand_batching_dims=(0,),
        start_indices_batching_dims=(0,),
    )
    return lax.gather(
        value, index[..., None], numbers, (1, 1), mode=lax.GatherScatterMode.PROMISE_IN_BOUNDS
    )


def kernel_table(gauss, lorentz, mixing, factor_ref):
    slots = gauss.shape[0]
    wing = (factor_ref.shape[1] - 1) // 2

    def profile(offset, factor):
        square = offset * offset
        width = lorentz * lorentz
        shape = mixing * (width / (square + width)) + (1.0 - mixing) * jnp.exp(
            -square / (2.0 * gauss * gauss)
        )
        return shape * factor

    lane = lax.broadcasted_iota(jnp.int32, (slots, LANES), 1)
    raw = []
    for start in range(0, 2 * wing, LANES):
        offset = (lane + (start - wing)).astype(jnp.float32)
        raw.append(profile(offset, factor_ref[:, start : start + LANES]))
    last = profile(jnp.full((slots, 1), float(wing), jnp.float32), factor_ref[:, 2 * wing :])
    total = jnp.sum(sum(raw), axis=1, keepdims=True) + last
    return jnp.concatenate(raw, axis=1) / total, last / total


def deposit_kernel(
    count_ref, bin_ref, slot_ref, strength_ref, gauss_ref, lorentz_ref, mixing_ref, factor_ref, give_ref, half_ref, acc_ref, spread_ref
):
    slots = gauss_ref.shape[1]
    pieces = (factor_ref.shape[1] - 1) // LANES
    lines = bin_ref.shape[1]
    reach_rows = (2 * HOP + 1) * SPAN // LANES
    rows = -(-reach_rows // 16) * 16
    bf16 = jnp.bfloat16

    table, last = kernel_table(
        column(gauss_ref[...]), column(lorentz_ref[...]), column(mixing_ref[...]), factor_ref
    )
    high, low = halves(table)
    weights = jnp.concatenate([high, low, high], axis=0)
    aux = lax.broadcasted_iota(jnp.int32, (16, LANES), 0)
    aux_lane = lax.broadcasted_iota(jnp.int32, (16, LANES), 1)
    steps = jnp.where(aux == 0, 1, jnp.where(aux == 1, LANES - aux_lane, 0))
    steps = steps.astype(jnp.float32).astype(bf16)
    weights = jnp.concatenate(
        [
            jnp.concatenate([weights, jnp.zeros((3 * slots, LANES), bf16)], axis=1),
            jnp.concatenate([jnp.zeros((16, table.shape[1]), bf16), steps], axis=1),
        ],
        axis=0,
    )

    anchor = (lax.axis_index("dev") - HOP) * SPAN
    count = count_ref[0]
    slot_ids = lax.broadcasted_iota(jnp.int32, (slots, STAGE), 0)
    row_ids = lax.broadcasted_iota(jnp.int32, (rows, BLOCK), 0)
    aux_ids = lax.broadcasted_iota(jnp.int32, (16, STAGE), 0)
    zero, one = jnp.zeros((BLOCK, LANES), bf16), jnp.ones((BLOCK, LANES), bf16)
    ends_at = []
    for start in range(0, lines, STAGE):
        at = slice(start, start + STAGE)
        col = (bin_ref[:, at] - anchor) & (LANES - 1)
        live = lax.broadcasted_iota(jnp.int32, (1, STAGE), 1) + start < count
        weight = jnp.where(live, strength_ref[:, at], 0.0)
        chosen = jnp.where(slot_ids == slot_ref[:, at], weight, 0.0)
        ends_at.append(jnp.sum(chosen * last, axis=0, keepdims=True))
        chosen_high, chosen_low = halves(chosen)
        aux = jnp.where(aux_ids == 0, col, jnp.where(aux_ids == 1, 1, 0))
        aux = aux.astype(jnp.float32).astype(bf16)
        picks = jnp.concatenate([chosen_high, chosen_high, chosen_low, aux], axis=0)
        spread_ref[at, :] = lax.dot_general(
            picks, weights, (((0,), (0,)), ((), ())), preferred_element_type=jnp.float32
        )
    ends_at = jnp.concatenate(ends_at, axis=1)
    acc = jnp.zeros((rows, 2 * (pieces + 1) * LANES), jnp.float32)
    ends = jnp.zeros((2 * rows, LANES), jnp.float32)
    for start in range(0, lines, BLOCK):
        at = slice(start, start + BLOCK)
        row = (bin_ref[:, at] - anchor) >> 7
        step = spread_ref[at, pieces * LANES :]
        index = step.astype(jnp.int32) & (LANES - 1)
        turned = [
            halves(pick_lanes(spread_ref[at, k * LANES : (k + 1) * LANES], index))
            for k in range(pieces)
        ]
        step = step.astype(bf16)
        after, here = step < LANES, step == LANES
        value = []
        for k in range(pieces + 1):
            past = turned[pieces - 1 - k] if k < pieces else (zero, zero)
            upto = turned[pieces - k] if k > 0 else (zero, zero)
            value += [jnp.where(after, a, b) for a, b in zip(past, upto)]
        chosen = row_ids == row
        onto = chosen.astype(jnp.float32).astype(bf16)
        acc += jnp.dot(
            onto, jnp.concatenate(value, axis=1), preferred_element_type=jnp.float32
        )
        onto = jnp.concatenate(halves(jnp.where(chosen, ends_at[:, at], 0.0)), axis=0)
        ends += jnp.dot(onto, jnp.where(here, one, zero), preferred_element_type=jnp.float32)

    span_rows, wing_rows = SPAN // LANES, pieces // 2
    shift = (HOP + 1) * span_rows - HOP * span_rows - wing_rows
    acc_ref[...] = jnp.zeros_like(acc_ref)
    acc_ref[shift : shift + rows] = ends[:rows] + ends[rows:]
    for k in range(pieces + 1):
        part = acc[:, 2 * k * LANES : (2 * k + 1) * LANES] + acc[:, (2 * k + 1) * LANES : 2 * (k + 1) * LANES]
        acc_ref[shift + k : shift + k + rows] += part
    odd = lax.rem(lax.axis_index(AXES), 2)
    far = HOP + 1
    give = pl.multiple_of((1 - odd) * (far + 1) * span_rows, span_rows)
    keep = pl.multiple_of(odd * far * span_rows, span_rows)
    give_ref[...] = acc_ref[pl.ds(give, far * span_rows)]
    half_ref[...] = acc_ref[pl.ds(keep, (far + 1) * span_rows)]


def span_sums(line_bin, line_slot, strength, line_count, gauss, lorentz, mixing, factor):
    lines, slots = line_bin.shape[0], gauss.shape[0]
    span_rows = SPAN // LANES
    rows = -(-((2 * HOP + 3) * span_rows + LANES) // 16) * 16
    vmem = pl.BlockSpec(memory_space=pltpu.VMEM)
    return pl.pallas_call(
        deposit_kernel,
        out_shape=[
            pltpu.VMEM(((HOP + 1) * span_rows, LANES), jnp.float32),
            pltpu.VMEM(((HOP + 2) * span_rows, LANES), jnp.float32),
        ],
        in_specs=[pl.BlockSpec(memory_space=pltpu.SMEM)] + [vmem] * 7,
        out_specs=[vmem] * 2,
        scratch_shapes=[
            pltpu.VMEM((rows, LANES), jnp.float32),
            pltpu.VMEM((lines, factor.shape[1] - 1 + LANES), jnp.float32),
        ],
    )(
        line_count,
        line_bin.reshape(1, lines),
        line_slot.reshape(1, lines),
        strength.reshape(1, lines),
        gauss.reshape(1, slots),
        lorentz.reshape(1, slots),
        mixing.reshape(1, slots),
        factor,
    )


def exchanges(groups, members):
    count = groups * members
    pair = [(i, i ^ 1) for i in range(count)]
    near, far, cross = [], [], []
    for i in range(count):
        step = 1 if i % 2 else -1
        end = 0 if i % 2 else members - 1
        for moves, j in ((near, i + step), (far, i + 3 * step)):
            if 0 <= j < count:
                if i // members == j // members:
                    moves.append((i, j))
                elif j % members == end:
                    (far if moves is far else cross).append((i, j))
    return pair, near, far, cross


def body(line_bin, line_slot, strength, line_count, gauss, lorentz, mixing, factor):
    groups, members = lax.axis_size("grp"), lax.axis_size("dev")
    pair, near, far, cross = exchanges(groups, members)
    rows = SPAN // LANES
    even = lax.axis_index("dev") % 2 == 0

    def part(value, first):
        return value[first * rows : (first + 1) * rows]

    give, half = span_sums(line_bin, line_slot, strength, line_count, gauss, lorentz, mixing, factor)
    got = lax.ppermute(give, AXES, pair)
    zero = jnp.zeros((rows, LANES), jnp.float32)
    half = half + jnp.where(
        even, jnp.concatenate([zero, got], axis=0), jnp.concatenate([got, zero], axis=0)
    )
    near = lax.ppermute(half[rows : 3 * rows], AXES, near)
    far = lax.ppermute(jnp.where(even, part(half, 0), part(half, 3)), AXES, far)
    cross = lax.ppermute(jnp.where(even, part(half, 2), part(half, 1)), AXES, cross)
    own = jnp.where(even, part(half, 3) + part(near, 0), part(half, 0) + part(near, 1))
    own = own + far + cross
    other = jnp.where(even, part(near, 1), part(near, 0))
    got = lax.ppermute(other, AXES, pair)
    return (own + got).reshape(SPAN)


def solution(mesh):
    in_specs = (P(AXES),) * 4 + (P(),) * 4
    return jax.shard_map(body, mesh=mesh, in_specs=in_specs, out_specs=P(AXES), check_vma=False)
```

```python
import jax
import jax.numpy as jnp
from jax import lax
from jax.experimental import pallas as pl
from jax.experimental.pallas import tpu as pltpu
from jax.sharding import PartitionSpec as P

HOP = 2
SPAN = 1024
LANES = 128
BLOCK = 128
STAGE = 512
AXES = ("grp", "dev")


def column(row):
    n = row.shape[1]
    here = lax.broadcasted_iota(jnp.int32, (n, n), 0)
    there = lax.broadcasted_iota(jnp.int32, (n, n), 1)
    return jnp.sum(jnp.where(here == there, row, 0.0), axis=1, keepdims=True)


def halves(value):
    high = value.astype(jnp.bfloat16)
    low = (value - high.astype(jnp.float32)).astype(jnp.bfloat16)
    return high, low


def pick_lanes(value, index):
    numbers = lax.GatherDimensionNumbers(
        offset_dims=(),
        collapsed_slice_dims=(1,),
        start_index_map=(1,),
        operand_batching_dims=(0,),
        start_indices_batching_dims=(0,),
    )
    return lax.gather(
        value, index[..., None], numbers, (1, 1), mode=lax.GatherScatterMode.PROMISE_IN_BOUNDS
    )


def kernel_table(gauss, lorentz, mixing, factor_ref):
    slots = gauss.shape[0]
    wing = (factor_ref.shape[1] - 1) // 2

    def profile(offset, factor):
        square = offset * offset
        width = lorentz * lorentz
        shape = mixing * (width / (square + width)) + (1.0 - mixing) * jnp.exp(
            -square / (2.0 * gauss * gauss)
        )
        return shape * factor

    lane = lax.broadcasted_iota(jnp.int32, (slots, LANES), 1)
    raw = []
    for start in range(0, 2 * wing, LANES):
        offset = (lane + (start - wing)).astype(jnp.float32)
        raw.append(profile(offset, factor_ref[:, start : start + LANES]))
    last = profile(jnp.full((slots, 1), float(wing), jnp.float32), factor_ref[:, 2 * wing :])
    total = jnp.sum(sum(raw), axis=1, keepdims=True) + last
    return jnp.concatenate(raw, axis=1) / total, last / total


def deposit_kernel(
    count_ref, bin_ref, slot_ref, strength_ref, gauss_ref, lorentz_ref, mixing_ref, factor_ref, give_ref, half_ref, acc_ref, spread_ref
):
    slots = gauss_ref.shape[1]
    pieces = (factor_ref.shape[1] - 1) // LANES
    lines = bin_ref.shape[1]
    reach_rows = (2 * HOP + 1) * SPAN // LANES
    rows = -(-reach_rows // 16) * 16
    bf16 = jnp.bfloat16

    table, last = kernel_table(
        column(gauss_ref[...]), column(lorentz_ref[...]), column(mixing_ref[...]), factor_ref
    )
    high, low = halves(table)
    weights = jnp.concatenate([high, low, high, low], axis=0)
    aux = lax.broadcasted_iota(jnp.int32, (16, LANES), 0)
    aux_lane = lax.broadcasted_iota(jnp.int32, (16, LANES), 1)
    steps = jnp.where(aux == 0, 1, jnp.where(aux == 1, LANES - aux_lane, 0))
    steps = steps.astype(jnp.float32).astype(bf16)
    weights = jnp.concatenate(
        [
            jnp.concatenate([weights, jnp.zeros((4 * slots, LANES), bf16)], axis=1),
            jnp.concatenate([jnp.zeros((16, table.shape[1]), bf16), steps], axis=1),
        ],
        axis=0,
    )

    anchor = (lax.axis_index("dev") - HOP) * SPAN
    count = count_ref[0]
    slot_ids = lax.broadcasted_iota(jnp.int32, (slots, STAGE), 0)
    row_ids = lax.broadcasted_iota(jnp.int32, (rows, BLOCK), 0)
    aux_ids = lax.broadcasted_iota(jnp.int32, (16, STAGE), 0)
    zero, one = jnp.zeros((BLOCK, LANES), bf16), jnp.ones((BLOCK, LANES), bf16)
    ends_at = []
    for start in range(0, lines, STAGE):
        at = slice(start, start + STAGE)
        col = (bin_ref[:, at] - anchor) & (LANES - 1)
        live = lax.broadcasted_iota(jnp.int32, (1, STAGE), 1) + start < count
        weight = jnp.where(live, strength_ref[:, at], 0.0)
        chosen = jnp.where(slot_ids == slot_ref[:, at], weight, 0.0)
        ends_at.append(jnp.sum(chosen * last, axis=0, keepdims=True))
        chosen_high, chosen_low = halves(chosen)
        aux = jnp.where(aux_ids == 0, col, jnp.where(aux_ids == 1, 1, 0))
        aux = aux.astype(jnp.float32).astype(bf16)
        picks = jnp.concatenate([chosen_high, chosen_high, chosen_low, chosen_low, aux], axis=0)
        spread_ref[at, :] = lax.dot_general(
            picks, weights, (((0,), (0,)), ((), ())), preferred_element_type=jnp.float32
        )
    ends_at = jnp.concatenate(ends_at, axis=1)
    acc = jnp.zeros((rows, 2 * (pieces + 1) * LANES), jnp.float32)
    ends = jnp.zeros((2 * rows, LANES), jnp.float32)
    for start in range(0, lines, BLOCK):
        at = slice(start, start + BLOCK)
        row = (bin_ref[:, at] - anchor) >> 7
        step = spread_ref[at, pieces * LANES :]
        index = step.astype(jnp.int32) & (LANES - 1)
        turned = [
            halves(pick_lanes(spread_ref[at, k * LANES : (k + 1) * LANES], index))
            for k in range(pieces)
        ]
        step = step.astype(bf16)
        after, here = step < LANES, step == LANES
        value = []
        for k in range(pieces + 1):
            past = turned[pieces - 1 - k] if k < pieces else (zero, zero)
            upto = turned[pieces - k] if k > 0 else (zero, zero)
            value += [jnp.where(after, a, b) for a, b in zip(past, upto)]
        chosen = row_ids == row
        onto = chosen.astype(jnp.float32).astype(bf16)
        acc += jnp.dot(
            onto, jnp.concatenate(value, axis=1), preferred_element_type=jnp.float32
        )
        onto = jnp.concatenate(halves(jnp.where(chosen, ends_at[:, at], 0.0)), axis=0)
        ends += jnp.dot(onto, jnp.where(here, one, zero), preferred_element_type=jnp.float32)

    span_rows, wing_rows = SPAN // LANES, pieces // 2
    shift = (HOP + 1) * span_rows - HOP * span_rows - wing_rows
    acc_ref[...] = jnp.zeros_like(acc_ref)
    acc_ref[shift : shift + rows] = ends[:rows] + ends[rows:]
    for k in range(pieces + 1):
        part = acc[:, 2 * k * LANES : (2 * k + 1) * LANES] + acc[:, (2 * k + 1) * LANES : 2 * (k + 1) * LANES]
        acc_ref[shift + k : shift + k + rows] += part
    odd = lax.rem(lax.axis_index(AXES), 2)
    far = HOP + 1
    give = pl.multiple_of((1 - odd) * (far + 1) * span_rows, span_rows)
    keep = pl.multiple_of(odd * far * span_rows, span_rows)
    give_ref[...] = acc_ref[pl.ds(give, far * span_rows)]
    half_ref[...] = acc_ref[pl.ds(keep, (far + 1) * span_rows)]


def span_sums(line_bin, line_slot, strength, line_count, gauss, lorentz, mixing, factor):
    lines, slots = line_bin.shape[0], gauss.shape[0]
    span_rows = SPAN // LANES
    rows = -(-((2 * HOP + 3) * span_rows + LANES) // 16) * 16
    vmem = pl.BlockSpec(memory_space=pltpu.VMEM)
    return pl.pallas_call(
        deposit_kernel,
        out_shape=[
            pltpu.VMEM(((HOP + 1) * span_rows, LANES), jnp.float32),
            pltpu.VMEM(((HOP + 2) * span_rows, LANES), jnp.float32),
        ],
        in_specs=[pl.BlockSpec(memory_space=pltpu.SMEM)] + [vmem] * 7,
        out_specs=[vmem] * 2,
        scratch_shapes=[
            pltpu.VMEM((rows, LANES), jnp.float32),
            pltpu.VMEM((lines, factor.shape[1] - 1 + LANES), jnp.float32),
        ],
    )(
        line_count,
        line_bin.reshape(1, lines),
        line_slot.reshape(1, lines),
        strength.reshape(1, lines),
        gauss.reshape(1, slots),
        lorentz.reshape(1, slots),
        mixing.reshape(1, slots),
        factor,
    )


def exchanges(groups, members):
    count = groups * members
    pair = [(i, i ^ 1) for i in range(count)]
    near, far, cross = [], [], []
    for i in range(count):
        step = 1 if i % 2 else -1
        end = 0 if i % 2 else members - 1
        for moves, j in ((near, i + step), (far, i + 3 * step)):
            if 0 <= j < count:
                if i // members == j // members:
                    moves.append((i, j))
                elif j % members == end:
                    (far if moves is far else cross).append((i, j))
    return pair, near, far, cross


def body(line_bin, line_slot, strength, line_count, gauss, lorentz, mixing, factor):
    groups, members = lax.axis_size("grp"), lax.axis_size("dev")
    pair, near, far, cross = exchanges(groups, members)
    rows = SPAN // LANES
    even = lax.axis_index("dev") % 2 == 0

    def part(value, first):
        return value[first * rows : (first + 1) * rows]

    give, half = span_sums(line_bin, line_slot, strength, line_count, gauss, lorentz, mixing, factor)
    got = lax.ppermute(give, AXES, pair)
    zero = jnp.zeros((rows, LANES), jnp.float32)
    half = half + jnp.where(
        even, jnp.concatenate([zero, got], axis=0), jnp.concatenate([got, zero], axis=0)
    )
    near = lax.ppermute(half[rows : 3 * rows], AXES, near)
    far = lax.ppermute(jnp.where(even, part(half, 0), part(half, 3)), AXES, far)
    cross = lax.ppermute(jnp.where(even, part(half, 2), part(half, 1)), AXES, cross)
    own = jnp.where(even, part(half, 3) + part(near, 0), part(half, 0) + part(near, 1))
    own = own + far + cross
    other = jnp.where(even, part(near, 1), part(near, 0))
    got = lax.ppermute(other, AXES, pair)
    return (own + got).reshape(SPAN)


def solution(mesh):
    in_specs = (P(AXES),) * 4 + (P(),) * 4
    return jax.shard_map(body, mesh=mesh, in_specs=in_specs, out_specs=P(AXES), check_vma=False)
```

```python
import jax
import jax.numpy as jnp
from jax import lax
from jax.experimental import pallas as pl
from jax.experimental.pallas import tpu as pltpu
from jax.sharding import PartitionSpec as P

HOP = 2
SPAN = 1024
LANES = 128
BLOCK = 256
STAGE = 256
AXES = ("grp", "dev")


def column(row):
    n = row.shape[1]
    here = lax.broadcasted_iota(jnp.int32, (n, n), 0)
    there = lax.broadcasted_iota(jnp.int32, (n, n), 1)
    return jnp.sum(jnp.where(here == there, row, 0.0), axis=1, keepdims=True)


def halves(value):
    high = value.astype(jnp.bfloat16)
    low = (value - high.astype(jnp.float32)).astype(jnp.bfloat16)
    return high, low


def pick_lanes(value, index):
    numbers = lax.GatherDimensionNumbers(
        offset_dims=(),
        collapsed_slice_dims=(1,),
        start_index_map=(1,),
        operand_batching_dims=(0,),
        start_indices_batching_dims=(0,),
    )
    return lax.gather(
        value, index[..., None], numbers, (1, 1), mode=lax.GatherScatterMode.PROMISE_IN_BOUNDS
    )


def kernel_table(gauss, lorentz, mixing, factor_ref):
    slots = gauss.shape[0]
    wing = (factor_ref.shape[1] - 1) // 2

    def profile(offset, factor):
        square = offset * offset
        width = lorentz * lorentz
        shape = mixing * (width / (square + width)) + (1.0 - mixing) * jnp.exp(
            -square / (2.0 * gauss * gauss)
        )
        return shape * factor

    lane = lax.broadcasted_iota(jnp.int32, (slots, LANES), 1)
    raw = []
    for start in range(0, 2 * wing, LANES):
        offset = (lane + (start - wing)).astype(jnp.float32)
        raw.append(profile(offset, factor_ref[:, start : start + LANES]))
    last = profile(jnp.full((slots, 1), float(wing), jnp.float32), factor_ref[:, 2 * wing :])
    total = sum(jnp.sum(part, axis=1, keepdims=True) for part in raw) + last
    return jnp.concatenate(raw, axis=1) / total, last / total


def deposit_kernel(
    count_ref, bin_ref, slot_ref, strength_ref, gauss_ref, lorentz_ref, mixing_ref, factor_ref, give_ref, half_ref, acc_ref, spread_ref
):
    slots = gauss_ref.shape[1]
    pieces = (factor_ref.shape[1] - 1) // LANES
    lines = bin_ref.shape[1]
    reach_rows = (2 * HOP + 1) * SPAN // LANES
    rows = -(-(reach_rows + pieces) // 16) * 16
    bf16 = jnp.bfloat16

    table, last = kernel_table(
        column(gauss_ref[...]), column(lorentz_ref[...]), column(mixing_ref[...]), factor_ref
    )
    high, low = halves(table)
    weights = jnp.concatenate([high, low, high, low], axis=0)
    aux = lax.broadcasted_iota(jnp.int32, (16, LANES), 0)
    aux_lane = lax.broadcasted_iota(jnp.int32, (16, LANES), 1)
    steps = jnp.where(aux == 0, 1, jnp.where(aux == 1, LANES - aux_lane, 0))
    steps = steps.astype(jnp.float32).astype(bf16)
    weights = jnp.concatenate(
        [
            jnp.concatenate([weights, jnp.zeros((4 * slots, LANES), bf16)], axis=1),
            jnp.concatenate([jnp.zeros((16, table.shape[1]), bf16), steps], axis=1),
        ],
        axis=0,
    )

    anchor = (lax.axis_index("dev") - HOP) * SPAN
    count = count_ref[0]
    slot_ids = lax.broadcasted_iota(jnp.int32, (slots, STAGE), 0)
    row_ids = lax.broadcasted_iota(jnp.int32, (rows, BLOCK), 0)
    aux_ids = lax.broadcasted_iota(jnp.int32, (16, STAGE), 0)
    zero, one = jnp.zeros((BLOCK, LANES), bf16), jnp.ones((BLOCK, LANES), bf16)
    ends_at = []
    for start in range(0, lines, STAGE):
        at = slice(start, start + STAGE)
        col = (bin_ref[:, at] - anchor) & (LANES - 1)
        live = lax.broadcasted_iota(jnp.int32, (1, STAGE), 1) + start < count
        weight = jnp.where(live, strength_ref[:, at], 0.0)
        chosen = jnp.where(slot_ids == slot_ref[:, at], weight, 0.0)
        ends_at.append(jnp.sum(chosen * last, axis=0, keepdims=True))
        chosen_high, chosen_low = halves(chosen)
        aux = jnp.where(aux_ids == 0, col, jnp.where(aux_ids == 1, 1, 0))
        aux = aux.astype(jnp.float32).astype(bf16)
        picks = jnp.concatenate([chosen_high, chosen_high, chosen_low, chosen_low, aux], axis=0)
        spread_ref[at, :] = lax.dot_general(
            picks, weights, (((0,), (0,)), ((), ())), preferred_element_type=jnp.float32
        )
    ends_at = jnp.concatenate(ends_at, axis=1)
    acc = jnp.zeros((rows, 2 * LANES), jnp.float32)
    ends = jnp.zeros((2 * rows, LANES), jnp.float32)
    for start in range(0, lines, BLOCK):
        at = slice(start, start + BLOCK)
        row = (bin_ref[:, at] - anchor) >> 7
        step = spread_ref[at, pieces * LANES :]
        index = step.astype(jnp.int32) & (LANES - 1)
        turned = [
            halves(pick_lanes(spread_ref[at, k * LANES : (k + 1) * LANES], index))
            for k in range(pieces)
        ]
        step = step.astype(bf16)
        after, here = step < LANES, step == LANES
        for k in range(pieces + 1):
            past = turned[pieces - 1 - k] if k < pieces else (zero, zero)
            upto = turned[pieces - k] if k > 0 else (zero, zero)
            value = [jnp.where(after, a, b) for a, b in zip(past, upto)]
            onto = (row_ids == row + k).astype(jnp.float32).astype(bf16)
            acc += jnp.dot(
                onto, jnp.concatenate(value, axis=1), preferred_element_type=jnp.float32
            )
        onto = jnp.concatenate(halves(jnp.where(row_ids == row, ends_at[:, at], 0.0)), axis=0)
        ends += jnp.dot(onto, jnp.where(here, one, zero), preferred_element_type=jnp.float32)
    acc = acc[:, :LANES] + acc[:, LANES:] + ends[:rows] + ends[rows:]

    span_rows, wing_rows = SPAN // LANES, pieces // 2
    shift = (HOP + 1) * span_rows - HOP * span_rows - wing_rows
    acc_ref[:shift] = jnp.zeros((shift, LANES), jnp.float32)
    acc_ref[shift : shift + rows] = acc
    end = shift + reach_rows + 2 * wing_rows
    acc_ref[end:] = jnp.zeros((acc_ref.shape[0] - end, LANES), jnp.float32)
    odd = lax.rem(lax.axis_index(AXES), 2)
    far = HOP + 1
    give = pl.multiple_of((1 - odd) * (far + 1) * span_rows, span_rows)
    keep = pl.multiple_of(odd * far * span_rows, span_rows)
    give_ref[...] = acc_ref[pl.ds(give, far * span_rows)]
    half_ref[...] = acc_ref[pl.ds(keep, (far + 1) * span_rows)]


def span_sums(line_bin, line_slot, strength, line_count, gauss, lorentz, mixing, factor):
    lines, slots = line_bin.shape[0], gauss.shape[0]
    span_rows = SPAN // LANES
    rows = -(-((2 * HOP + 3) * span_rows + LANES) // 16) * 16
    vmem = pl.BlockSpec(memory_space=pltpu.VMEM)
    return pl.pallas_call(
        deposit_kernel,
        out_shape=[
            pltpu.VMEM(((HOP + 1) * span_rows, LANES), jnp.float32),
            pltpu.VMEM(((HOP + 2) * span_rows, LANES), jnp.float32),
        ],
        in_specs=[pl.BlockSpec(memory_space=pltpu.SMEM)] + [vmem] * 7,
        out_specs=[vmem] * 2,
        scratch_shapes=[
            pltpu.VMEM((rows, LANES), jnp.float32),
            pltpu.VMEM((lines, factor.shape[1] - 1 + LANES), jnp.float32),
        ],
    )(
        line_count,
        line_bin.reshape(1, lines),
        line_slot.reshape(1, lines),
        strength.reshape(1, lines),
        gauss.reshape(1, slots),
        lorentz.reshape(1, slots),
        mixing.reshape(1, slots),
        factor,
    )


def exchanges(groups, members):
    count = groups * members
    pair = [(i, i ^ 1) for i in range(count)]
    near, far, cross = [], [], []
    for i in range(count):
        step = 1 if i % 2 else -1
        end = 0 if i % 2 else members - 1
        for moves, j in ((near, i + step), (far, i + 3 * step)):
            if 0 <= j < count:
                if i // members == j // members:
                    moves.append((i, j))
                elif j % members == end:
                    (far if moves is far else cross).append((i, j))
    return pair, near, far, cross


def body(line_bin, line_slot, strength, line_count, gauss, lorentz, mixing, factor):
    groups, members = lax.axis_size("grp"), lax.axis_size("dev")
    pair, near, far, cross = exchanges(groups, members)
    rows = SPAN // LANES
    even = lax.axis_index("dev") % 2 == 0

    def part(value, first):
        return value[first * rows : (first + 1) * rows]

    give, half = span_sums(line_bin, line_slot, strength, line_count, gauss, lorentz, mixing, factor)
    got = lax.ppermute(give, AXES, pair)
    far = lax.ppermute(jnp.where(even, part(half, 0), part(half, 3)), AXES, far)
    zero = jnp.zeros((rows, LANES), jnp.float32)
    half = half + jnp.where(
        even, jnp.concatenate([zero, got], axis=0), jnp.concatenate([got, zero], axis=0)
    )
    near = lax.ppermute(half[rows : 3 * rows], AXES, near)
    cross = lax.ppermute(jnp.where(even, part(half, 2), part(half, 1)), AXES, cross)
    own = jnp.where(even, part(half, 3) + part(near, 0), part(half, 0) + part(near, 1))
    own = own + far + cross
    other = jnp.where(even, part(near, 1), part(near, 0))
    got = lax.ppermute(other, AXES, pair)
    return (own + got).reshape(SPAN)


def solution(mesh):
    in_specs = (P(AXES),) * 4 + (P(),) * 4
    return jax.shard_map(body, mesh=mesh, in_specs=in_specs, out_specs=P(AXES), check_vma=False)
```
